256 devices in a mesh: trial: 4 (over z_lo), ep: 4 (over y), fsdp: 16 (over z_hi, x, core).
Axes of the slice: x: 4, y: 4, z: 8 (z_hi: 2, z_lo: 4; z = z_hi * 4 + z_lo), core: 2. Of those that a mesh axis runs over, the one named last changes fastest.
Arguments:
- master_down: float32 [256, 1024, 2048], P(('trial', 'ep'), None, 'fsdp'), parts along dimension 0, may hold values from -0.25 to 0.25
- router_weight: float32 [8192, 64], P(('trial', 'fsdp'), 'ep'), parts along dimension 0, may hold values from -0.125 to 0.125
- router_gain: float32 [8192], P(('trial', 'fsdp')), parts along dimension 0, may hold values from 0.25 to 1.75
Outputs:
- final_down: bfloat16 [256, 1024, 2048], P(('trial', 'ep'), 'fsdp'), parts along dimension 0
- scale_down: float32 [256, 1024], P(('trial', 'ep'), 'fsdp'), parts along dimension 0
- serve_router: bfloat16 [8192, 64], P('trial'), parts along dimension 0
The draws below stay inside these ranges and needn't reach their ends.
There are 4 independent parts, one for each index of `trial`. The reference program is written for one: setup_inputs(seed, part) draws one part's arguments, and reference() takes and returns one part's arrays. A program takes and returns all parts, laid end to end along the dimension named above; each array names one. Nothing has to cross between parts.
All inputs are finite; a program needn't handle non-finite values. Where the reference program divides by a largest or mean magnitude, that divisor is 1e-20 or more.
Results may differ from the reference program's by a relative error of at most 0.001.
Values may be sent and summed in bfloat16 or wider, within the bound.
A program may use at most 64 MiB of HBM per device.

```python
import jax
import jax.numpy as jnp

EXPERTS = 64
D_MODEL = 2048
D_EXPERT = 1024


def strengthened(array, key, source, target, shards_of, factor):
    def block_of(position):
        return (jnp.arange(array.shape[position]) // (array.shape[position] // shards_of)).reshape((-1,) + (1,) * (array.ndim - 1 - position))

    first = jax.random.permutation(key, shards_of)[block_of(target)]
    second = (block_of(target) + shards_of // 2) % shards_of
    return jnp.where((block_of(source) == first) | (block_of(source) == second), factor * array, array)


def block_scale(own_key, dims, cuts, smallest, largest):
    level = 1.0
    for axis_at, shards_of in cuts:
        draws = jax.random.uniform(jax.random.fold_in(jax.random.fold_in(own_key, 6), axis_at), (shards_of,), jnp.float32, smallest / len(cuts), largest / len(cuts))
        level = level * jnp.repeat(jnp.exp(draws), dims[axis_at] // shards_of).reshape((-1,) + (1,) * (len(dims) - 1 - axis_at))
    return level


def centred(own_key, shape, scale, bound, pieces=(), kind=jnp.bfloat16):
    result = jax.random.normal(own_key, shape, jnp.float32) * scale
    if len(pieces) > 0:
        result = block_scale(own_key, shape, pieces, -0.22, 0.18) * result
    return jnp.clip(result, min=-bound, max=bound).astype(kind)


def bell_draw_with(rng, extent, deviation, reach, split, heavy, kind=jnp.bfloat16):
    result = deviation * jax.random.normal(rng, extent, jnp.float32)
    if split:
        result = result * block_scale(rng, extent, split, -0.22, 0.18)
    return jnp.clip(strengthened(result, jax.random.fold_in(rng, 3), *heavy), -reach, reach).astype(kind)


def setup_inputs(seed: int = 0, part: int = 0) -> dict:
    arg_keys = jax.random.split(jax.random.key(seed), 4)
    part_splits = jax.random.split(jax.random.fold_in(arg_keys[3], part), 4)
    master_down = bell_draw_with(part_splits[0], (EXPERTS, D_EXPERT, D_MODEL), D_EXPERT ** -0.5, 0.25, ((0, 4), (2, 16)), (2, 1, 16, 2.0), jnp.float32)
    router_weight = centred(part_splits[1], (D_MODEL, EXPERTS), D_MODEL ** -0.5, 0.125, ((0, 16), (1, 4)), jnp.float32)
    router_gain = jnp.clip(1.0 + 0.15 * jax.random.normal(part_splits[2], (D_MODEL,), jnp.float32), 0.25, 1.75)
    return dict(master_down=master_down, router_weight=router_weight, router_gain=router_gain)


def reference(master_down, router_weight, router_gain):
    scale_down = jnp.max(jnp.abs(master_down), axis=2)
    final_down = (master_down / jnp.expand_dims(scale_down, 2)).astype(jnp.bfloat16)
    serve_router = (router_weight * router_gain[:, None]).astype(jnp.bfloat16)
    return final_down, scale_down, serve_router
```

```python
import functools

import jax
import jax.numpy as jnp
from jax import lax
from jax.experimental import pallas as pl
from jax.experimental.pallas import tpu as pltpu
from jax.sharding import PartitionSpec as P

MESH = pl.DeviceIdType.MESH

OFFSETS = [(1, dx, dc) for dx in (0, 1, 3, 2) for dc in (0, 1)] + [
    (0, dx, dc) for dx in (1, 3, 2, 0) for dc in (0, 1) if (dx, dc) != (0, 0)
]
SAME_CORE = [o for o in OFFSETS if o[2] == 0]
FIRST = 2
STEP = 2


def kernel(
    experts,
    rows,
    w_hbm,
    rt_ref,
    gain_ref,
    final_ref,
    scale_ref,
    router_ref,
    w,
    narrow,
    maxima,
    straight,
    paired,
    partner,
    others,
    scales,
    own_router,
    load_sem,
    send_sem,
    recv_sem,
    straight_send,
    straight_recv,
    pair_send,
    pair_recv,
    other_send,
    other_recv,
    back_send,
    back_recv,
    router_send,
    router_recv,
):
    trial, ep, me = lax.axis_index("trial"), lax.axis_index("ep"), lax.axis_index("fsdp")
    plane, x, core = me // 8, lax.rem(me // 2, 4), lax.rem(me, 2)
    share = rows // 16

    def at(offset, sign=1):
        dz, dx, dc = offset
        return lax.rem(plane + dz, 2) * 8 + lax.rem(x + 4 + sign * dx, 4) * 2 + lax.rem(core + dc, 2)

    def send(src, dst, send, recv, index, row=None):
        return pltpu.make_async_remote_copy(
            src_ref=src,
            dst_ref=dst,
            send_sem=send,
            recv_sem=recv,
            device_id=(trial, ep if row is None else row, index),
            device_id_type=MESH,
        )

    def columns(index):
        return pl.ds(pl.multiple_of(index * 128, 128), 128)

    loads = [pltpu.make_async_copy(w_hbm.at[e], w.at[e], load_sem.at[e]) for e in range(experts)]
    for load in loads:
        load.start()

    barrier = pltpu.get_barrier_semaphore()
    for o in OFFSETS:
        pl.semaphore_signal(barrier, inc=1, device_id=(trial, ep, at(o)), device_id_type=MESH)
    for d in (1, 2, 3):
        pl.semaphore_signal(barrier, inc=1, device_id=(trial, lax.rem(ep + d, 4), me), device_id_type=MESH)

    part = (rt_ref[...] * gain_ref[...]).astype(jnp.bfloat16)
    own_router[...] = part
    own_rows = pl.ds(pl.multiple_of(ep * 16, 16), 16)
    router_ref[own_rows, columns(me)] = part

    def take_maxima(e):
        for b in range(rows // 128):
            block = jnp.abs(w[e, b * 128 : (b + 1) * 128, :])
            maxima[e, b : b + 1, :] = jnp.max(block.T, axis=0, keepdims=True)

    def divide(e):
        inverse = 1.0 / scales[e]
        for b in range(rows // 128):
            factor = jnp.broadcast_to(inverse[b : b + 1, :], (128, 128)).T
            narrow[e, b * 128 : (b + 1) * 128, :] = (w[e, b * 128 : (b + 1) * 128, :] * factor).astype(jnp.bfloat16)

    for e in range(FIRST):
        loads[e].wait()
        take_maxima(e)
    pl.semaphore_wait(barrier, len(OFFSETS) + 3)

    straights = [
        send(maxima.at[pl.ds(0, FIRST)], straight.at[i], straight_send.at[i], straight_recv.at[i], at(o))
        for i, o in enumerate(OFFSETS)
    ]
    for s in straights:
        s.start()
    router_y = [
        send(own_router, router_ref.at[own_rows, columns(me)], router_send.at[d - 1], router_recv.at[d - 1], me, lax.rem(ep + d, 4))
        for d in (1, 2, 3)
    ]
    for s in router_y:
        s.start()

    half = (experts - FIRST) // 2
    mine = pl.ds(FIRST + core * half, half)
    theirs = pl.ds(FIRST + (1 - core) * half, half)
    for e in range(FIRST, experts):
        loads[e].wait()

    def later_maxima(e, carry):
        take_maxima(e)
        return carry

    lax.fori_loop(FIRST, experts, later_maxima, 0)
    pair = send(maxima.at[theirs], partner, pair_send, pair_recv, at((0, 0, 1)))
    pair.start()
    for s in router_y:
        s.wait()
    router_x = [
        send(
            router_ref.at[:, columns(me)],
            router_ref.at[:, columns(me)],
            router_send.at[3 + i],
            router_recv.at[3 + i],
            at(o),
        )
        for i, o in enumerate(SAME_CORE)
    ]
    for s in router_x:
        s.start()
    pair.wait()
    paired[...] = jnp.maximum(maxima[mine], partner[...])
    exchange = [
        send(paired, others.at[i], other_send.at[i], other_recv.at[i], at(o)) for i, o in enumerate(SAME_CORE)
    ]
    for s in exchange:
        s.start()

    top = maxima[0:FIRST]
    for s in straights:
        s.wait()
    for i in range(len(OFFSETS)):
        top = jnp.maximum(top, straight[i])
    scales[0:FIRST] = top

    def parcels(k):
        block = pl.ds(k * STEP, STEP)
        return [
            send(
                narrow.at[block, pl.ds(pl.multiple_of(at(o) * share, share), share), :],
                final_ref.at[block, :, columns(me)],
                send_sem.at[i],
                recv_sem.at[i],
                at(o),
            )
            for i, o in enumerate(OFFSETS)
        ]

    def step(k, carry):
        for e in range(STEP):
            divide(k * STEP + e)

        @pl.when(k > 0)
        def _():
            for s in parcels(k):
                s.wait_send()

        for s in parcels(k):
            s.start()
        for e in range(STEP):
            final_ref[k * STEP + e, :, columns(me)] = narrow[
                k * STEP + e, pl.ds(pl.multiple_of(me * share, share), share), :
            ]
        return carry

    lax.fori_loop(0, FIRST // STEP, step, 0)

    for s in exchange:
        s.wait()
    top = paired[...]
    for i in range(len(SAME_CORE)):
        top = jnp.maximum(top, others[i])
    scales[mine] = top
    back = send(scales.at[mine], scales.at[mine], back_send, back_recv, at((0, 0, 1)))
    back.start()
    back.wait()

    lax.fori_loop(FIRST // STEP, experts // STEP, step, 0)

    for s in router_x:
        s.wait()
    router_core = []
    for i in range(8):
        column = columns(i * 2 + core)
        router_core.append(
            send(router_ref.at[:, column], router_ref.at[:, column], router_send.at[10 + i], router_recv.at[10 + i], at((0, 0, 1)))
        )
    for s in router_core:
        s.start()
    ours = scales[:, pl.ds(me // 2, 1), :].reshape(experts, 128)
    scale_ref[...] = jnp.where(core == 0, ours[:, :share], ours[:, share:])
    for s in router_core:
        s.wait()
    for s in parcels(0):
        s.wait_send()
    for i, o in enumerate(OFFSETS):
        whole = final_ref.at[:, :, columns(at(o, -1))]
        send(whole, whole, send_sem.at[i], recv_sem.at[i], at(o)).wait_recv()


def solution(mesh):
    def shards(master_down, router_weight, router_gain):
        experts, rows, _ = master_down.shape
        half = (experts - FIRST) // 2
        peers, cores = len(OFFSETS), len(SAME_CORE)
        vmem = pl.BlockSpec(memory_space=pltpu.VMEM)
        dma = pltpu.SemaphoreType.DMA
        final_down, scale_down, router = pl.pallas_call(
            functools.partial(kernel, experts, rows),
            out_shape=(
                jax.ShapeDtypeStruct((experts, rows // 16, 2048), jnp.bfloat16),
                jax.ShapeDtypeStruct((experts, rows // 16), jnp.float32),
                jax.ShapeDtypeStruct((64, 2048), jnp.bfloat16),
            ),
            in_specs=[pl.BlockSpec(memory_space=pl.ANY), vmem, vmem],
            out_specs=(vmem, vmem, vmem),
            scratch_shapes=[
                pltpu.VMEM((experts, rows, 128), jnp.float32),
                pltpu.VMEM((experts, rows, 128), jnp.bfloat16),
                pltpu.VMEM((experts, 8, 128), jnp.float32),
                pltpu.VMEM((peers, FIRST, 8, 128), jnp.float32),
                pltpu.VMEM((half, 8, 128), jnp.float32),
                pltpu.VMEM((half, 8, 128), jnp.float32),
                pltpu.VMEM((cores, half, 8, 128), jnp.float32),
                pltpu.VMEM((experts, 8, 128), jnp.float32),
                pltpu.VMEM((16, 128), jnp.bfloat16),
                dma((experts,)),
                dma((peers,)),
                dma((peers,)),
                dma((peers,)),
                dma((peers,)),
                dma,
                dma,
                dma((cores,)),
                dma((cores,)),
                dma,
                dma,
                dma((18,)),
                dma((18,)),
            ],
            compiler_params=pltpu.CompilerParams(
                collective_id=0, has_side_effects=True, vmem_limit_bytes=48 * 2**20
            ),
            name="serve",
        )(master_down, router_weight.T, router_gain[None, :])
        return final_down, scale_down, router.T

    return jax.shard_map(
        shards,
        mesh=mesh,
        in_specs=(
            P(("trial", "ep"), None, "fsdp"),
            P(("trial", "fsdp"), "ep"),
            P(("trial", "fsdp")),
        ),
        out_specs=(P(("trial", "ep"), "fsdp", None), P(("trial", "ep"), "fsdp"), P("trial", None)),
        check_vma=False,
    )
```

```python
import functools

import jax
import jax.numpy as jnp
from jax import lax
from jax.experimental import pallas as pl
from jax.experimental.pallas import tpu as pltpu
from jax.sharding import PartitionSpec as P

MESH = pl.DeviceIdType.MESH

OFFSETS = [(1, dx, dc) for dx in (0, 1, 3, 2) for dc in (0, 1)] + [
    (0, dx, dc) for dx in (1, 3, 2, 0) for dc in (0, 1) if (dx, dc) != (0, 0)
]
ALONG_X = [(0, dx, 0) for dx in (1, 3, 2)]
ACROSS_Z = (1, 0, 0)
PARTNER = (0, 0, 1)
FIRST = 2
GROUPS = ((2, 8), (8, 16))
RAW = 4
STEP = 2


def kernel(
    experts,
    rows,
    w_hbm,
    rt_hbm,
    gain_hbm,
    final_ref,
    scale_ref,
    router_ref,
    w,
    narrow,
    raw,
    maxima,
    straight,
    partner,
    paired,
    along,
    planed,
    across,
    scales,
    rt,
    gain,
    own_router,
    load_sem,
    send_sem,
    recv_sem,
    raw_send,
    raw_recv,
    straight_send,
    straight_recv,
    pair_send,
    pair_recv,
    along_send,
    along_recv,
    across_send,
    across_recv,
    back_send,
    back_recv,
    router_send,
    router_recv,
):
    trial, ep, me = lax.axis_index("trial"), lax.axis_index("ep"), lax.axis_index("fsdp")
    plane, x, core = me // 8, lax.rem(me // 2, 4), lax.rem(me, 2)
    share = rows // 16
    last = experts - 1

    def at(offset, sign=1):
        dz, dx, dc = offset
        return lax.rem(plane + dz, 2) * 8 + lax.rem(x + 4 + sign * dx, 4) * 2 + lax.rem(core + dc, 2)

    def send(src, dst, send, recv, index, row=None):
        return pltpu.make_async_remote_copy(
            src_ref=src,
            dst_ref=dst,
            send_sem=send,
            recv_sem=recv,
            device_id=(trial, ep if row is None else row, index),
            device_id_type=MESH,
        )

    def columns(index):
        return pl.ds(pl.multiple_of(index * 128, 128), 128)

    def part_of(index):
        return pl.ds(pl.multiple_of(index * share, share), share)

    barrier = pltpu.get_barrier_semaphore()
    for o in OFFSETS:
        pl.semaphore_signal(barrier, inc=1, device_id=(trial, ep, at(o)), device_id_type=MESH)
    for d in (1, 2, 3):
        pl.semaphore_signal(barrier, inc=1, device_id=(trial, lax.rem(ep + d, 4), me), device_id_type=MESH)

    loads = [pltpu.make_async_copy(w_hbm.at[e], w.at[e], load_sem.at[e]) for e in range(experts)]
    rt_load = pltpu.make_async_copy(rt_hbm, rt, load_sem.at[experts])
    gain_load = pltpu.make_async_copy(gain_hbm, gain, load_sem.at[experts + 1])
    for e in range(FIRST):
        loads[e].start()
    rt_load.start()
    gain_load.start()
    loads[last].start()
    for e in range(FIRST, last):
        loads[e].start()

    def take_maxima(e):
        for b in range(rows // 128):
            block = jnp.abs(w[e, b * 128 : (b + 1) * 128, :])
            maxima[e, b : b + 1, :] = jnp.max(block.T, axis=0, keepdims=True)

    def divide(e):
        inverse = 1.0 / scales[e]
        for b in range(rows // 128):
            factor = jnp.broadcast_to(inverse[b : b + 1, :], (128, 128)).T
            narrow[e, b * 128 : (b + 1) * 128, :] = (w[e, b * 128 : (b + 1) * 128, :] * factor).astype(jnp.bfloat16)

    def maxima_of(lo, hi):
        def one(e, carry):
            take_maxima(e)
            return carry

        lax.fori_loop(lo, hi, one, 0)

    with jax.named_scope("first_maxima"):
        for e in range(FIRST):
            loads[e].wait()
        maxima_of(0, FIRST)
    with jax.named_scope("router_part"):
        rt_load.wait()
        gain_load.wait()
        part = (rt[...] * gain[...]).astype(jnp.bfloat16)
        own_router[...] = part
        own_rows = pl.ds(pl.multiple_of(ep * 16, 16), 16)
        router_ref[own_rows, columns(me)] = part
    with jax.named_scope("maxima_a"):
        for e in range(FIRST, experts):
            loads[e].wait()
        maxima_of(*GROUPS[0])
    with jax.named_scope("barrier_wait"):
        pl.semaphore_wait(barrier, len(OFFSETS) + 3)

    straights = [
        send(maxima.at[pl.ds(0, FIRST)], straight.at[i], straight_send.at[i], straight_recv.at[i], at(o))
        for i, o in enumerate(OFFSETS)
    ]
    for s in straights:
        s.start()

    halves, kept, taken = [], [], 0
    for lo, hi in GROUPS:
        half = (hi - lo) // 2
        halves.append((pl.ds(lo + core * half, half), pl.ds(lo + (1 - core) * half, half)))
        kept.append(pl.ds(taken, half))
        taken += half
    pairs = [
        send(maxima.at[theirs], partner.at[k], pair_send.at[g], pair_recv.at[g], at(PARTNER))
        for g, ((_, theirs), k) in enumerate(zip(halves, kept))
    ]
    alongs = [
        [
            send(paired.at[k], along.at[i, k], along_send.at[g, i], along_recv.at[g, i], at(o))
            for i, o in enumerate(ALONG_X)
        ]
        for g, k in enumerate(kept)
    ]
    acrosses = [
        send(planed.at[k], across.at[k], across_send.at[g], across_recv.at[g], at(ACROSS_Z))
        for g, k in enumerate(kept)
    ]
    backs = [
        send(scales.at[mine], scales.at[mine], back_send.at[g], back_recv.at[g], at(PARTNER))
        for g, (mine, _) in enumerate(halves)
    ]
    raws = [
        send(w.at[last, part_of(at(o)), :], raw.at[i], raw_send.at[i], raw_recv.at[i], at(o))
        for i, o in enumerate(OFFSETS[:RAW])
    ]

    pairs[0].start()
    for s in raws:
        s.start()
    router_y = [
        send(own_router, router_ref.at[own_rows, columns(me)], router_send.at[d - 1], router_recv.at[d - 1], me, lax.rem(ep + d, 4))
        for d in (1, 2, 3)
    ]
    for s in router_y:
        s.start()

    def reduce_pair(g):
        pairs[g].wait()
        paired[kept[g]] = jnp.maximum(maxima[halves[g][0]], partner[kept[g]])
        for s in alongs[g]:
            s.start()

    def reduce_along(g):
        for s in alongs[g]:
            s.wait()
        top = paired[kept[g]]
        for i in range(len(ALONG_X)):
            top = jnp.maximum(top, along[i, kept[g]])
        planed[kept[g]] = top
        acrosses[g].start()

    def reduce_across(g):
        acrosses[g].wait()
        scales[halves[g][0]] = jnp.maximum(planed[kept[g]], across[kept[g]])
        backs[g].start()

    with jax.named_scope("pair_a"):
        reduce_pair(0)
    with jax.named_scope("maxima_b"):
        maxima_of(*GROUPS[1])
        pairs[1].start()
    with jax.named_scope("router_y"):
        for s in router_y:
            s.wait()
    router_x = [
        send(router_ref.at[:, columns(me)], router_ref.at[:, columns(me)], router_send.at[3 + i], router_recv.at[3 + i], at(o))
        for i, o in enumerate(ALONG_X + [ACROSS_Z])
    ]
    for s in router_x:
        s.start()
    with jax.named_scope("pair_b"):
        reduce_pair(1)
    with jax.named_scope("along_a"):
        reduce_along(0)
    with jax.named_scope("along_b"):
        reduce_along(1)

    with jax.named_scope("straight_wait"):
        for s in straights:
            s.wait()
        top = maxima[0:FIRST]
        for i in range(len(OFFSETS)):
            top = jnp.maximum(top, straight[i])
        scales[0:FIRST] = top

    def parcel(block, i, slot):
        o = OFFSETS[i]
        return send(
            narrow.at[block, part_of(at(o)), :],
            final_ref.at[block, :, columns(me)],
            send_sem.at[slot, i],
            recv_sem.at[i],
            at(o),
        )

    peers = range(len(OFFSETS))

    def keep(e):
        final_ref[e, :, columns(me)] = narrow[e, part_of(me), :]

    def step(k, carry):
        block = pl.ds(k * STEP, STEP)
        slot = lax.rem(k, 2)
        with jax.named_scope("divide"):
            for e in range(STEP):
                divide(k * STEP + e)

        with jax.named_scope("send_wait"):
            @pl.when(k > 1)
            def _():
                for i in peers:
                    parcel(block, i, slot).wait_send()

        for i in peers:
            parcel(block, i, slot).start()
        for e in range(STEP):
            keep(k * STEP + e)
        return carry

    lax.fori_loop(0, FIRST // STEP, step, 0)
    for g in range(len(GROUPS)):
        with jax.named_scope(f"across_{g}"):
            reduce_across(g)
    for g in range(len(GROUPS)):
        with jax.named_scope(f"back_{g}"):
            backs[g].wait()
    steps = experts // STEP
    lax.fori_loop(FIRST // STEP, steps - 1, step, 0)

    for e in range(STEP):
        divide(experts - STEP + e)
    end = (steps - 1) % 2
    for i in peers:
        parcel(pl.ds(0, STEP), i, end).wait_send()
    ends = [parcel(pl.ds(experts - STEP, STEP - 1 if i < RAW else STEP), i, end) for i in peers]
    for s in ends:
        s.start()
    for e in range(STEP):
        keep(experts - STEP + e)

    ours = scales[:, pl.ds(me // 2, 1), :].reshape(experts, 128)
    scale_ref[...] = jnp.where(core == 0, ours[:, :share], ours[:, share:])
    factor = jnp.broadcast_to(1.0 / ours[last:], (128, 128)).T
    factor = jnp.where(core == 0, factor[:share], factor[share:])
    for i in range(RAW):
        raws[i].wait()
        final_ref[last, :, columns(at(OFFSETS[i], -1))] = (raw[i] * factor).astype(jnp.bfloat16)

    with jax.named_scope("router_x"):
        for s in router_x:
            s.wait()
    sides = [at(o) for o in ALONG_X] + [me]
    across_z = lax.rem(me + 8, 16)
    router_far = [
        send(router_ref.at[:, columns(across_z)], router_ref.at[:, columns(across_z)], router_send.at[7 + i], router_recv.at[7 + i], at(o))
        for i, o in enumerate(ALONG_X)
    ]
    for s in router_far:
        s.start()
    for s in router_far:
        s.wait()
    router_core = []
    for i in range(8):
        column = columns(i * 2 + core)
        router_core.append(
            send(router_ref.at[:, column], router_ref.at[:, column], router_send.at[10 + i], router_recv.at[10 + i], at(PARTNER))
        )
    for s in router_core:
        s.start()
    for s in router_core:
        s.wait()
    with jax.named_scope("last_waits"):
        for i in peers:
            parcel(pl.ds(0, STEP), i, 1 - end).wait_send()
            ends[i].wait_send()
        for i, o in enumerate(OFFSETS):
            whole = final_ref.at[pl.ds(0, last if i < RAW else experts), :, columns(at(o, -1))]
            send(whole, whole, send_sem.at[0, i], recv_sem.at[i], at(o)).wait_recv()


def place(final_in, scale_in, router_in, final_out, scale_out, router_out, sem):
    copies = [
        pltpu.make_async_copy(src, dst, sem.at[i])
        for i, (src, dst) in enumerate(((final_in, final_out), (scale_in, scale_out), (router_in, router_out)))
    ]
    for c in copies:
        c.start()
    for c in copies:
        c.wait()


def solution(mesh):
    def shards(master_down, router_weight, router_gain):
        experts, rows, _ = master_down.shape
        held = sum(hi - lo for lo, hi in GROUPS) // 2
        peers, groups, sides = len(OFFSETS), len(GROUPS), len(ALONG_X)
        vmem = pl.BlockSpec(memory_space=pltpu.VMEM)
        hbm = pl.BlockSpec(memory_space=pltpu.HBM)
        dma = pltpu.SemaphoreType.DMA
        shapes = (
            jax.ShapeDtypeStruct((experts, rows // 16, 2048), jnp.bfloat16),
            jax.ShapeDtypeStruct((experts, rows // 16), jnp.float32),
            jax.ShapeDtypeStruct((64, 2048), jnp.bfloat16),
        )
        tile = (8, 128)
        results = pl.pallas_call(
            functools.partial(kernel, experts, rows),
            out_shape=shapes,
            in_specs=[hbm] * 3,
            out_specs=(vmem, vmem, vmem),
            scratch_shapes=[
                pltpu.VMEM((experts, rows, 128), jnp.float32),
                pltpu.VMEM((experts, rows, 128), jnp.bfloat16),
                pltpu.VMEM((RAW, rows // 16, 128), jnp.float32),
                pltpu.VMEM((experts, *tile), jnp.float32),
                pltpu.VMEM((peers, FIRST, *tile), jnp.float32),
                pltpu.VMEM((held, *tile), jnp.float32),
                pltpu.VMEM((held, *tile), jnp.float32),
                pltpu.VMEM((sides, held, *tile), jnp.float32),
                pltpu.VMEM((held, *tile), jnp.float32),
                pltpu.VMEM((held, *tile), jnp.float32),
                pltpu.VMEM((experts, *tile), jnp.float32),
                pltpu.VMEM((16, 128), jnp.float32),
                pltpu.VMEM((1, 128), jnp.float32),
                pltpu.VMEM((16, 128), jnp.bfloat16),
                dma((experts + 2,)),
                dma((2, peers)),
                dma((peers,)),
                dma((RAW,)),
                dma((RAW,)),
                dma((peers,)),
                dma((peers,)),
                dma((groups,)),
                dma((groups,)),
                dma((groups, sides)),
                dma((groups, sides)),
                dma((groups,)),
                dma((groups,)),
                dma((groups,)),
                dma((groups,)),
                dma((18,)),
                dma((18,)),
            ],
            compiler_params=pltpu.CompilerParams(
                collective_id=0, has_side_effects=True, vmem_limit_bytes=48 * 2**20
            ),
            name="serve",
        )(master_down, *(pltpu.with_memory_space_constraint(a, pltpu.HBM) for a in (router_weight.T, router_gain[None, :])))
        final_down, scale_down, router = pl.pallas_call(
            place,
            out_shape=shapes,
            in_specs=[pl.BlockSpec(memory_space=pl.ANY)] * 3,
            out_specs=(hbm,) * 3,
            scratch_shapes=[dma((3,))],
            compiler_params=pltpu.CompilerParams(vmem_limit_bytes=8 * 2**20),
            name="place",
        )(*results)
        return final_down, scale_down, router.T

    return jax.shard_map(
        shards,
        mesh=mesh,
        in_specs=(
            P(("trial", "ep"), None, "fsdp"),
            P(("trial", "fsdp"), "ep"),
            P(("trial", "fsdp")),
        ),
        out_specs=(P(("trial", "ep"), "fsdp", None), P(("trial", "ep"), "fsdp"), P("trial", None)),
        check_vma=False,
    )
```

```python
import functools

import jax
import jax.numpy as jnp
from jax import lax
from jax.experimental import pallas as pl
from jax.experimental.pallas import tpu as pltpu
from jax.sharding import PartitionSpec as P

MESH = pl.DeviceIdType.MESH

OFFSETS = [(1, dx, dc) for dx in (0, 1, 3, 2) for dc in (0, 1)] + [
    (0, dx, dc) for dx in (1, 3, 2, 0) for dc in (0, 1) if (dx, dc) != (0, 0)
]
ALONG_X = [(0, dx, 0) for dx in (1, 3, 2)]
ACROSS_Z = (1, 0, 0)
PARTNER = (0, 0, 1)
ACROSS = OFFSETS[:8]
FIRST = 3
RAW = (2, 4)
WINDOW = 4
LEFT = 2


def kernel(
    experts,
    rows,
    w_hbm,
    rt_hbm,
    gain_hbm,
    final_ref,
    scale_ref,
    router_ref,
    w,
    narrow,
    raw,
    maxima,
    straight,
    early,
    partner,
    paired,
    along,
    planed,
    across,
    scales,
    rt,
    gain,
    own_router,
    load_sem,
    send_sem,
    recv_sem,
    raw_send,
    raw_recv,
    straight_send,
    straight_recv,
    pair_send,
    pair_recv,
    along_send,
    along_recv,
    across_send,
    across_recv,
    back_send,
    back_recv,
    router_send,
    router_recv,
    go,
    gate,
):
    trial, ep, me = lax.axis_index("trial"), lax.axis_index("ep"), lax.axis_index("fsdp")
    z_first = trial < 2
    plane, x, core = me // 8, lax.rem(me // 2, 4), lax.rem(me, 2)
    share = rows // 16
    last = experts - 1

    def at(offset, sign=1):
        dz, dx, dc = offset
        return lax.rem(plane + dz, 2) * 8 + lax.rem(x + 4 + sign * dx, 4) * 2 + lax.rem(core + dc, 2)

    def send(src, dst, send, recv, index, row=None):
        return pltpu.make_async_remote_copy(
            src_ref=src,
            dst_ref=dst,
            send_sem=send,
            recv_sem=recv,
            device_id=(trial, ep if row is None else row, index),
            device_id_type=MESH,
        )

    def columns(index):
        return pl.ds(pl.multiple_of(index * 128, 128), 128)

    def part_of(index):
        return pl.ds(pl.multiple_of(index * share, share), share)

    barrier = pltpu.get_barrier_semaphore()
    for o in OFFSETS:
        pl.semaphore_signal(barrier, inc=1, device_id=(trial, ep, at(o)), device_id_type=MESH)
    for d in (1, 2, 3):
        pl.semaphore_signal(barrier, inc=1, device_id=(trial, lax.rem(ep + d, 4), me), device_id_type=MESH)
    sharers = [(lax.rem(trial + 2, 4), ep, at(o)) for o in ((0, 0, 0), ACROSS_Z)]
    gated = lax.rem(me + 8 * lax.rem(trial, 2), 16)
    for d in sharers:
        pl.semaphore_signal(barrier, inc=1, device_id=d, device_id_type=MESH)

    loads = [pltpu.make_async_copy(w_hbm.at[e], w.at[e], load_sem.at[e]) for e in range(experts)]
    rt_load = pltpu.make_async_copy(rt_hbm, rt, load_sem.at[experts])
    gain_load = pltpu.make_async_copy(gain_hbm, gain, load_sem.at[experts + 1])
    for e in range(FIRST):
        loads[e].start()
    rt_load.start()
    gain_load.start()
    loads[last].start()
    for e in range(FIRST, last):
        loads[e].start()

    def take_maxima(e):
        for b in range(rows // 128):
            block = jnp.abs(w[e, b * 128 : (b + 1) * 128, :])
            maxima[e, b : b + 1, :] = jnp.max(block.T, axis=0, keepdims=True)

    def divide(e, scale):
        inverse = 1.0 / scale
        for b in range(rows // 128):
            factor = jnp.broadcast_to(inverse[b : b + 1, :], (128, 128)).T
            narrow[e, b * 128 : (b + 1) * 128, :] = (w[e, b * 128 : (b + 1) * 128, :] * factor).astype(jnp.bfloat16)

    def maxima_of(lo, hi):
        def one(e, carry):
            pltpu.make_async_copy(w_hbm.at[e], w.at[e], load_sem.at[e]).wait()
            take_maxima(e)
            return carry

        lax.fori_loop(lo, hi, one, 0)

    with jax.named_scope("first_maxima"):
        maxima_of(0, FIRST)
    with jax.named_scope("router_part"):
        rt_load.wait()
        gain_load.wait()
        part = (rt[...] * gain[...]).astype(jnp.bfloat16)
        own_router[...] = part
        own_rows = pl.ds(pl.multiple_of(ep * 16, 16), 16)
        router_ref[own_rows, columns(me)] = part
    loads[last].wait()

    def other_maxima():
        with jax.named_scope("other_maxima"):
            maxima_of(FIRST, last)
            take_maxima(last)

    straights = [
        send(maxima.at[pl.ds(0, FIRST)], straight.at[i], straight_send, straight_recv, at(o))
        for i, o in enumerate(OFFSETS)
    ]
    raws = [
        send(w.at[last, part_of(at(o)), :], raw.at[i], raw_send, raw_recv, at(o))
        for i, o in enumerate(ACROSS)
    ]
    router_y = [
        send(own_router, router_ref.at[own_rows, columns(me)], router_send.at[0], router_recv.at[0], me, lax.rem(ep + d, 4))
        for d in (1, 2, 3)
    ]
    router_z = send(own_router, router_ref.at[own_rows, columns(me)], router_send.at[1], router_recv.at[1], at(ACROSS_Z))
    half = experts // 2
    mine, theirs = pl.ds(core * half, half), pl.ds((1 - core) * half, half)
    pair = send(maxima.at[theirs], partner, pair_send, pair_recv, at(PARTNER))
    along_x = [send(planed, along.at[i], along_send, along_recv, at(o)) for i, o in enumerate(ALONG_X)]
    across_z = send(paired, across, across_send, across_recv, at(ACROSS_Z))
    back = send(scales.at[mine], scales.at[mine], back_send, back_recv, at(PARTNER))

    @pl.when(jnp.logical_not(z_first))
    def _():
        other_maxima()

    with jax.named_scope("barrier_wait"):
        pl.semaphore_wait(barrier, len(OFFSETS) + 3 + len(sharers))

    @pl.when(z_first)
    def _():
        for s in straights + raws[: RAW[0]] + router_y + [router_z]:
            s.start()
        other_maxima()
        pair.start()

    @pl.when(jnp.logical_not(z_first))
    def _():
        for s in [pair] + router_y + [router_z]:
            s.start()

    with jax.named_scope("pair"):
        pair.wait()
        paired[...] = jnp.maximum(maxima[mine], partner[...])
    across_z.start()

    @pl.when(jnp.logical_not(z_first))
    def _():
        with jax.named_scope("gate_open"):
            across_z.wait_send()
            router_z.wait_send()
            pl.semaphore_signal(gate, inc=1, device_id=(lax.rem(trial + 2, 4), ep, gated), device_id_type=MESH)
            for s in raws[: RAW[1]]:
                s.start()

    everyone = list(enumerate(OFFSETS))
    far, near = everyone[:8], everyone[8:]

    def parcel(e, i, o):
        block = pl.ds(e, 1)
        return send(
            narrow.at[block, part_of(at(o)), :],
            final_ref.at[block, :, columns(me)],
            send_sem.at[lax.rem(e, WINDOW), i // 8],
            recv_sem.at[i],
            at(o),
        )

    def await_sent(e, which):
        if which:
            size = narrow.at[0, pl.ds(0, share * len(which)), :]
            send(size, size, send_sem.at[lax.rem(e, WINDOW), which[0][0] // 8], recv_sem.at[0], me).wait_send()

    def step(e, which):
        with jax.named_scope("send_wait"):
            if not isinstance(e, int):
                @pl.when(e >= WINDOW)
                def _():
                    await_sent(e, which)

        for i, o in which:
            parcel(e, i, o).start()

    def fresh(e, scale):
        with jax.named_scope("divide"):
            divide(e, scale)
        final_ref[e, :, columns(me)] = narrow[e, part_of(me), :]

    def steps(lo, hi, which, first):
        def one(e, carry):
            if first:
                fresh(e, scales[e])
            step(e, which)
            return carry

        lax.fori_loop(lo, hi, one, 0)

    @pl.when(z_first)
    def _():
        with jax.named_scope("straight_wait"):
            send(straight, straight, straight_send, straight_recv, me).wait()
            top = maxima[0:FIRST]
            for i in range(len(OFFSETS)):
                top = jnp.maximum(top, straight[i])
            early[...] = top
        for e in range(FIRST):
            fresh(e, early[e])
        with jax.named_scope("gate_wait"):
            pl.semaphore_wait(gate, 1)
        for e in range(FIRST):
            step(e, far)
        across_z.wait_send()

    with jax.named_scope("across"):
        across_z.wait_recv()
        planed[...] = jnp.maximum(paired[...], across[...])
    for s in along_x:
        s.start()
    with jax.named_scope("along"):
        send(along, along, along_send, along_recv, me).wait()
        top = planed[...]
        for i in range(len(ALONG_X)):
            top = jnp.maximum(top, along[i])
        scales[mine] = top
    back.start()
    with jax.named_scope("back"):
        back.wait()

    ours = scales[:, pl.ds(me // 2, 1), :].reshape(experts, 128)
    scale_ref[...] = jnp.where(core == 0, ours[:, :share], ours[:, share:])

    opposite = lax.rem(me + 8, 16)
    theirs_y = router_ref.at[own_rows, columns(opposite)]
    router_y2 = [
        send(theirs_y, theirs_y, router_send.at[2], router_recv.at[2], me, lax.rem(ep + d, 4)) for d in (1, 2, 3)
    ]
    router_x = [
        send(router_ref.at[:, columns(c)], router_ref.at[:, columns(c)], router_send.at[3], router_recv.at[3], at(o))
        for c in (me, opposite)
        for o in ALONG_X
    ]
    router_core = [
        send(router_ref.at[:, columns(c)], router_ref.at[:, columns(c)], router_send.at[4], router_recv.at[4], at(PARTNER))
        for c in [i * 2 + core for i in range(8)]
    ]

    def finish_router():
        with jax.named_scope("router_rest"):
            def arrived(which, blocks, columns_of):
                size = router_ref.at[pl.ds(0, 16 * blocks), pl.ds(0, 128 * columns_of)]
                send(size, size, router_send.at[which], router_recv.at[which], me).wait()

            arrived(0, 3, 1)
            router_z.wait_recv()
            for s in router_y2:
                s.start()
            arrived(2, 3, 1)
            for s in router_x:
                s.start()
            arrived(3, 4, 6)
            for s in router_core:
                s.start()
            arrived(4, 4, 8)

    def take_raw(count):
        with jax.named_scope("raw"):
            factor = jnp.broadcast_to(1.0 / ours[last:], (128, 128)).T
            factor = jnp.where(core == 0, factor[:share], factor[share:])
            if count:
                size = raw.at[pl.ds(0, count)]
                send(size, size, raw_send, raw_recv, me).wait()
            for i, o in enumerate(ACROSS[:count]):
                final_ref[last, :, columns(at(o, -1))] = (raw[i] * factor).astype(jnp.bfloat16)

    def received(which, count):
        for i, o in which:
            whole = final_ref.at[pl.ds(0, count), :, columns(at(o, -1))]
            send(whole, whole, send_sem.at[0, 0], recv_sem.at[i], at(o)).wait_recv()

    @pl.when(z_first)
    def _():
        with jax.named_scope("far_first"):
            steps(FIRST, last, far, True)
            fresh(last, scales[last])
            await_sent(last - WINDOW, far)
            for i, o in far[RAW[0] :]:
                parcel(last, i, o).start()
        with jax.named_scope("far_sent"):
            router_z.wait_send()
            for e in range(last - WINDOW + 1, last - LEFT + 1):
                await_sent(e, far)
            for d in sharers:
                pl.semaphore_signal(go, inc=1, device_id=d, device_id_type=MESH)
        take_raw(RAW[0])
        finish_router()
        with jax.named_scope("near_second"):
            steps(0, experts, near, False)
        with jax.named_scope("last_sends"):
            for e in range(last - LEFT + 1, last):
                await_sent(e, far)
            await_sent(last, far[RAW[0] :])
            for e in range(experts - WINDOW, experts):
                await_sent(e, near)
        with jax.named_scope("last_far"):
            received(far[: RAW[0]], last)
            received(far[RAW[0] :], experts)

    @pl.when(jnp.logical_not(z_first))
    def _():
        with jax.named_scope("near_first"):
            steps(0, experts, near, True)
        finish_router()
        with jax.named_scope("go_wait"):
            pl.semaphore_wait(go, len(sharers))
        with jax.named_scope("far_second"):
            steps(0, last, far, False)
            await_sent(last - WINDOW, far)
            for i, o in far[RAW[1] :]:
                parcel(last, i, o).start()
        take_raw(RAW[1])
        with jax.named_scope("last_sends"):
            for e in range(experts - WINDOW, experts):
                await_sent(e, near)
            for e in range(last - WINDOW + 1, last):
                await_sent(e, far)
            await_sent(last, far[RAW[1] :])
        with jax.named_scope("last_far"):
            received(far[: RAW[1]], last)
            received(far[RAW[1] :], experts)

    with jax.named_scope("last_near"):
        received(near, experts)


def place(final_in, scale_in, router_in, final_out, scale_out, router_out, sem):
    copies = [
        pltpu.make_async_copy(src, dst, sem.at[i])
        for i, (src, dst) in enumerate(((final_in, final_out), (scale_in, scale_out), (router_in, router_out)))
    ]
    for c in copies:
        c.start()
    for c in copies:
        c.wait()


def solution(mesh):
    def shards(master_down, router_weight, router_gain):
        experts, rows, _ = master_down.shape
        held = experts // 2
        peers, sides = len(OFFSETS), len(ALONG_X)
        vmem = pl.BlockSpec(memory_space=pltpu.VMEM)
        hbm = pl.BlockSpec(memory_space=pltpu.HBM)
        dma = pltpu.SemaphoreType.DMA
        shapes = (
            jax.ShapeDtypeStruct((experts, rows // 16, 2048), jnp.bfloat16),
            jax.ShapeDtypeStruct((experts, rows // 16), jnp.float32),
            jax.ShapeDtypeStruct((64, 2048), jnp.bfloat16),
        )
        tile = (8, 128)
        results = pl.pallas_call(
            functools.partial(kernel, experts, rows),
            out_shape=shapes,
            in_specs=[hbm] * 3,
            out_specs=(vmem, vmem, vmem),
            scratch_shapes=[
                pltpu.VMEM((experts, rows, 128), jnp.float32),
                pltpu.VMEM((experts, rows, 128), jnp.bfloat16),
                pltpu.VMEM((len(ACROSS), rows // 16, 128), jnp.float32),
                pltpu.VMEM((experts, *tile), jnp.float32),
                pltpu.VMEM((peers, FIRST, *tile), jnp.float32),
                pltpu.VMEM((FIRST, *tile), jnp.float32),
                pltpu.VMEM((held, *tile), jnp.float32),
                pltpu.VMEM((held, *tile), jnp.float32),
                pltpu.VMEM((sides, held, *tile), jnp.float32),
                pltpu.VMEM((held, *tile), jnp.float32),
                pltpu.VMEM((held, *tile), jnp.float32),
                pltpu.VMEM((experts, *tile), jnp.float32),
                pltpu.VMEM((16, 128), jnp.float32),
                pltpu.VMEM((1, 128), jnp.float32),
                pltpu.VMEM((16, 128), jnp.bfloat16),
                dma((experts + 2,)),
                dma((WINDOW, 2)),
                dma((peers,)),
                *[dma] * 12,
                dma((5,)),
                dma((5,)),
                pltpu.SemaphoreType.REGULAR,
                pltpu.SemaphoreType.REGULAR,
            ],
            compiler_params=pltpu.CompilerParams(
                collective_id=0, has_side_effects=True, vmem_limit_bytes=48 * 2**20
            ),
            name="serve",
        )(master_down, *(pltpu.with_memory_space_constraint(a, pltpu.HBM) for a in (router_weight.T, router_gain[None, :])))
        final_down, scale_down, router = pl.pallas_call(
            place,
            out_shape=shapes,
            in_specs=[pl.BlockSpec(memory_space=pl.ANY)] * 3,
            out_specs=(hbm,) * 3,
            scratch_shapes=[dma((3,))],
            compiler_params=pltpu.CompilerParams(vmem_limit_bytes=8 * 2**20),
            name="place",
        )(*results)
        return final_down, scale_down, router.T

    return jax.shard_map(
        shards,
        mesh=mesh,
        in_specs=(
            P(("trial", "ep"), None, "fsdp"),
            P(("trial", "fsdp"), "ep"),
            P(("trial", "fsdp")),
        ),
        out_specs=(P(("trial", "ep"), "fsdp", None), P(("trial", "ep"), "fsdp"), P("trial", None)),
        check_vma=False,
    )
```

```python
import functools

import jax
import jax.numpy as jnp
from jax import lax
from jax.experimental import pallas as pl
from jax.experimental.pallas import tpu as pltpu
from jax.sharding import PartitionSpec as P

MESH = pl.DeviceIdType.MESH

OFFSETS = [(1, dx, dc) for dx in (2, 1, 3, 0) for dc in (0, 1)] + [
    (0, dx, dc) for dx in (1, 3, 2, 0) for dc in (0, 1) if (dx, dc) != (0, 0)
]
ALONG_X = [(0, dx, 0) for dx in (1, 3, 2)]
ACROSS_Z = (1, 0, 0)
PARTNER = (0, 0, 1)
ACROSS = OFFSETS[:8]
FIRST = 3
RAW = (2, 1)
WINDOW = 4
LEFT = 2


def kernel(
    experts,
    rows,
    w_hbm,
    rt_hbm,
    gain_hbm,
    final_ref,
    scale_ref,
    router_ref,
    w,
    narrow,
    raw,
    maxima,
    straight,
    early,
    partner,
    paired,
    along,
    planed,
    across,
    scales,
    rt,
    gain,
    own_router,
    load_sem,
    send_sem,
    recv_sem,
    raw_send,
    raw_recv,
    straight_send,
    straight_recv,
    pair_send,
    pair_recv,
    along_send,
    along_recv,
    across_send,
    across_recv,
    back_send,
    back_recv,
    router_send,
    router_recv,
    go,
    gate,
):
    trial, ep, me = lax.axis_index("trial"), lax.axis_index("ep"), lax.axis_index("fsdp")
    z_first = trial < 2
    plane, x, core = me // 8, lax.rem(me // 2, 4), lax.rem(me, 2)
    share = rows // 16
    last = experts - 1

    def at(offset, sign=1):
        dz, dx, dc = offset
        return lax.rem(plane + dz, 2) * 8 + lax.rem(x + 4 + sign * dx, 4) * 2 + lax.rem(core + dc, 2)

    def send(src, dst, send, recv, index, row=None):
        return pltpu.make_async_remote_copy(
            src_ref=src,
            dst_ref=dst,
            send_sem=send,
            recv_sem=recv,
            device_id=(trial, ep if row is None else row, index),
            device_id_type=MESH,
        )

    def columns(index):
        return pl.ds(pl.multiple_of(index * 128, 128), 128)

    def part_of(index):
        return pl.ds(pl.multiple_of(index * share, share), share)

    barrier = pltpu.get_barrier_semaphore()
    for o in OFFSETS:
        pl.semaphore_signal(barrier, inc=1, device_id=(trial, ep, at(o)), device_id_type=MESH)
    for d in (1, 2, 3):
        pl.semaphore_signal(barrier, inc=1, device_id=(trial, lax.rem(ep + d, 4), me), device_id_type=MESH)
    sharers = [(lax.rem(trial + 2, 4), ep, at(o)) for o in ((0, 0, 0), ACROSS_Z)]
    gated = lax.rem(me + 8 * lax.rem(trial, 2), 16)
    for d in sharers:
        pl.semaphore_signal(barrier, inc=1, device_id=d, device_id_type=MESH)

    loads = [pltpu.make_async_copy(w_hbm.at[e], w.at[e], load_sem.at[e]) for e in range(experts)]
    rt_load = pltpu.make_async_copy(rt_hbm, rt, load_sem.at[experts])
    gain_load = pltpu.make_async_copy(gain_hbm, gain, load_sem.at[experts + 1])
    for e in range(FIRST):
        loads[e].start()
    rt_load.start()
    gain_load.start()
    loads[last].start()
    for e in range(FIRST, last):
        loads[e].start()

    def take_maxima(e):
        for b in range(rows // 128):
            block = jnp.abs(w[e, b * 128 : (b + 1) * 128, :])
            maxima[e, b : b + 1, :] = jnp.max(block.T, axis=0, keepdims=True)

    def divide(e, scale):
        inverse = 1.0 / scale
        for b in range(rows // 128):
            factor = jnp.broadcast_to(inverse[b : b + 1, :], (128, 128)).T
            narrow[e, b * 128 : (b + 1) * 128, :] = (w[e, b * 128 : (b + 1) * 128, :] * factor).astype(jnp.bfloat16)

    def maxima_of(lo, hi):
        def one(e, carry):
            pltpu.make_async_copy(w_hbm.at[e], w.at[e], load_sem.at[e]).wait()
            take_maxima(e)
            return carry

        lax.fori_loop(lo, hi, one, 0)

    with jax.named_scope("first_maxima"):
        maxima_of(0, FIRST)
    with jax.named_scope("router_part"):
        rt_load.wait()
        gain_load.wait()
        part = (rt[...] * gain[...]).astype(jnp.bfloat16)
        own_router[...] = part
        own_rows = pl.ds(pl.multiple_of(ep * 16, 16), 16)
        router_ref[own_rows, columns(me)] = part
    loads[last].wait()

    def other_maxima():
        with jax.named_scope("other_maxima"):
            maxima_of(FIRST, last)
            take_maxima(last)

    straights = [
        send(maxima.at[pl.ds(0, FIRST)], straight.at[i], straight_send, straight_recv, at(o))
        for i, o in enumerate(OFFSETS)
    ]
    raws = [
        send(w.at[last, part_of(at(o)), :], raw.at[i], raw_send, raw_recv, at(o))
        for i, o in enumerate(ACROSS)
    ]
    router_y = [
        send(own_router, router_ref.at[own_rows, columns(me)], router_send.at[0], router_recv.at[0], me, lax.rem(ep + d, 4))
        for d in (1, 2, 3)
    ]
    router_z = send(own_router, router_ref.at[own_rows, columns(me)], router_send.at[1], router_recv.at[1], at(ACROSS_Z))
    half = experts // 2
    mine, theirs = pl.ds(core * half, half), pl.ds((1 - core) * half, half)
    pair = send(maxima.at[theirs], partner, pair_send, pair_recv, at(PARTNER))
    along_x = [send(planed, along.at[i], along_send, along_recv, at(o)) for i, o in enumerate(ALONG_X)]
    across_z = send(paired, across, across_send, across_recv, at(ACROSS_Z))
    back = send(scales.at[mine], scales.at[mine], back_send, back_recv, at(PARTNER))

    @pl.when(jnp.logical_not(z_first))
    def _():
        other_maxima()

    with jax.named_scope("barrier_wait"):
        pl.semaphore_wait(barrier, len(OFFSETS) + 3 + len(sharers))

    @pl.when(z_first)
    def _():
        for s in straights + raws[: RAW[0]] + router_y + [router_z]:
            s.start()
        other_maxima()
        pair.start()

    @pl.when(jnp.logical_not(z_first))
    def _():
        for s in [pair] + router_y + [router_z]:
            s.start()

    with jax.named_scope("pair"):
        pair.wait()
        paired[...] = jnp.maximum(maxima[mine], partner[...])
    across_z.start()

    @pl.when(jnp.logical_not(z_first))
    def _():
        with jax.named_scope("gate_open"):
            across_z.wait_send()
            router_z.wait_send()
            pl.semaphore_signal(gate, inc=1, device_id=(lax.rem(trial + 2, 4), ep, gated), device_id_type=MESH)
            for s in raws[: RAW[1]]:
                s.start()

    everyone = list(enumerate(OFFSETS))
    far, near = everyone[:8], everyone[8:]

    def parcel(e, i, o):
        block = pl.ds(e, 1)
        return send(
            narrow.at[block, part_of(at(o)), :],
            final_ref.at[block, :, columns(me)],
            send_sem.at[lax.rem(e, WINDOW), i // 8],
            recv_sem.at[i],
            at(o),
        )

    def await_sent(e, which):
        if which:
            size = narrow.at[0, pl.ds(0, share * len(which)), :]
            send(size, size, send_sem.at[lax.rem(e, WINDOW), which[0][0] // 8], recv_sem.at[0], me).wait_send()

    def step(e, which):
        with jax.named_scope("send_wait"):
            if not isinstance(e, int):
                @pl.when(e >= WINDOW)
                def _():
                    await_sent(e, which)

        for i, o in which:
            parcel(e, i, o).start()

    def fresh(e, scale):
        with jax.named_scope("divide"):
            divide(e, scale)
        final_ref[e, :, columns(me)] = narrow[e, part_of(me), :]

    def steps(lo, hi, which, first):
        def one(e, carry):
            if first:
                fresh(e, scales[e])
            step(e, which)
            return carry

        lax.fori_loop(lo, hi, one, 0)

    @pl.when(z_first)
    def _():
        with jax.named_scope("straight_wait"):
            send(straight, straight, straight_send, straight_recv, me).wait()
            top = maxima[0:FIRST]
            for i in range(len(OFFSETS)):
                top = jnp.maximum(top, straight[i])
            early[...] = top
        fresh(0, early[0])
        with jax.named_scope("gate_wait"):
            pl.semaphore_wait(gate, 1)
        step(0, far)
        for e in range(1, FIRST):
            fresh(e, early[e])
            step(e, far)
        across_z.wait_send()

    with jax.named_scope("across"):
        across_z.wait_recv()
        planed[...] = jnp.maximum(paired[...], across[...])
    for s in along_x:
        s.start()
    with jax.named_scope("along"):
        send(along, along, along_send, along_recv, me).wait()
        top = planed[...]
        for i in range(len(ALONG_X)):
            top = jnp.maximum(top, along[i])
        scales[mine] = top
    back.start()
    with jax.named_scope("back"):
        back.wait()

    ours = scales[:, pl.ds(me // 2, 1), :].reshape(experts, 128)
    scale_ref[...] = jnp.where(core == 0, ours[:, :share], ours[:, share:])

    opposite = lax.rem(me + 8, 16)
    theirs_y = router_ref.at[own_rows, columns(opposite)]
    router_y2 = [
        send(theirs_y, theirs_y, router_send.at[2], router_recv.at[2], me, lax.rem(ep + d, 4)) for d in (1, 2, 3)
    ]
    router_x = [
        send(router_ref.at[:, columns(c)], router_ref.at[:, columns(c)], router_send.at[3], router_recv.at[3], at(o))
        for c in (me, opposite)
        for o in ALONG_X
    ]
    router_core = [
        send(router_ref.at[:, columns(c)], router_ref.at[:, columns(c)], router_send.at[4], router_recv.at[4], at(PARTNER))
        for c in [i * 2 + core for i in range(8)]
    ]

    def finish_router():
        with jax.named_scope("router_rest"):
            def arrived(which, blocks, columns_of):
                size = router_ref.at[pl.ds(0, 16 * blocks), pl.ds(0, 128 * columns_of)]
                send(size, size, router_send.at[which], router_recv.at[which], me).wait()

            arrived(0, 3, 1)
            router_z.wait_recv()
            for s in router_y2:
                s.start()
            arrived(2, 3, 1)
            for s in router_x:
                s.start()
            arrived(3, 4, 6)
            for s in router_core:
                s.start()
            arrived(4, 4, 8)

    def take_raw(count):
        with jax.named_scope("raw"):
            factor = jnp.broadcast_to(1.0 / ours[last:], (128, 128)).T
            factor = jnp.where(core == 0, factor[:share], factor[share:])
            if count:
                size = raw.at[pl.ds(0, count)]
                send(size, size, raw_send, raw_recv, me).wait()
            for i, o in enumerate(ACROSS[:count]):
                final_ref[last, :, columns(at(o, -1))] = (raw[i] * factor).astype(jnp.bfloat16)

    def received(which, count):
        for i, o in which:
            whole = final_ref.at[pl.ds(0, count), :, columns(at(o, -1))]
            send(whole, whole, send_sem.at[0, 0], recv_sem.at[i], at(o)).wait_recv()

    @pl.when(z_first)
    def _():
        with jax.named_scope("far_first"):
            steps(FIRST, last, far, True)
            fresh(last, scales[last])
            await_sent(last - WINDOW, far)
            for i, o in far[RAW[0] :]:
                parcel(last, i, o).start()
        with jax.named_scope("far_sent"):
            router_z.wait_send()
            for e in range(last - WINDOW + 1, last - LEFT + 1):
                await_sent(e, far)
            for d in sharers:
                pl.semaphore_signal(go, inc=1, device_id=d, device_id_type=MESH)
        take_raw(RAW[0])
        finish_router()
        with jax.named_scope("near_second"):
            steps(0, experts, near, False)
        with jax.named_scope("last_sends"):
            for e in range(last - LEFT + 1, last):
                await_sent(e, far)
            await_sent(last, far[RAW[0] :])
            for e in range(experts - WINDOW, experts):
                await_sent(e, near)
        with jax.named_scope("last_far"):
            received(far[: RAW[0]], last)
            received(far[RAW[0] :], experts)

    @pl.when(jnp.logical_not(z_first))
    def _():
        with jax.named_scope("near_first"):
            steps(0, experts, near, True)
        finish_router()
        with jax.named_scope("go_wait"):
            pl.semaphore_wait(go, len(sharers))
        with jax.named_scope("far_second"):
            steps(0, last, far, False)
            await_sent(last - WINDOW, far)
            for i, o in far[RAW[1] :]:
                parcel(last, i, o).start()
        take_raw(RAW[1])
        with jax.named_scope("last_sends"):
            for e in range(experts - WINDOW, experts):
                await_sent(e, near)
            for e in range(last - WINDOW + 1, last):
                await_sent(e, far)
            await_sent(last, far[RAW[1] :])
        with jax.named_scope("last_far"):
            received(far[: RAW[1]], last)
            received(far[RAW[1] :], experts)

    with jax.named_scope("last_near"):
        received(near, experts)


def place(final_in, scale_in, router_in, final_out, scale_out, router_out, sem):
    copies = [
        pltpu.make_async_copy(src, dst, sem.at[i])
        for i, (src, dst) in enumerate(((final_in, final_out), (scale_in, scale_out), (router_in, router_out)))
    ]
    for c in copies:
        c.start()
    for c in copies:
        c.wait()


def solution(mesh):
    def shards(master_down, router_weight, router_gain):
        experts, rows, _ = master_down.shape
        held = experts // 2
        peers, sides = len(OFFSETS), len(ALONG_X)
        vmem = pl.BlockSpec(memory_space=pltpu.VMEM)
        hbm = pl.BlockSpec(memory_space=pltpu.HBM)
        dma = pltpu.SemaphoreType.DMA
        shapes = (
            jax.ShapeDtypeStruct((experts, rows // 16, 2048), jnp.bfloat16),
            jax.ShapeDtypeStruct((experts, rows // 16), jnp.float32),
            jax.ShapeDtypeStruct((64, 2048), jnp.bfloat16),
        )
        tile = (8, 128)
        results = pl.pallas_call(
            functools.partial(kernel, experts, rows),
            out_shape=shapes,
            in_specs=[hbm] * 3,
            out_specs=(vmem, vmem, vmem),
            scratch_shapes=[
                pltpu.VMEM((experts, rows, 128), jnp.float32),
                pltpu.VMEM((experts, rows, 128), jnp.bfloat16),
                pltpu.VMEM((len(ACROSS), rows // 16, 128), jnp.float32),
                pltpu.VMEM((experts, *tile), jnp.float32),
                pltpu.VMEM((peers, FIRST, *tile), jnp.float32),
                pltpu.VMEM((FIRST, *tile), jnp.float32),
                pltpu.VMEM((held, *tile), jnp.float32),
                pltpu.VMEM((held, *tile), jnp.float32),
                pltpu.VMEM((sides, held, *tile), jnp.float32),
                pltpu.VMEM((held, *tile), jnp.float32),
                pltpu.VMEM((held, *tile), jnp.float32),
                pltpu.VMEM((experts, *tile), jnp.float32),
                pltpu.VMEM((16, 128), jnp.float32),
                pltpu.VMEM((1, 128), jnp.float32),
                pltpu.VMEM((16, 128), jnp.bfloat16),
                dma((experts + 2,)),
                dma((WINDOW, 2)),
                dma((peers,)),
                *[dma] * 12,
                dma((5,)),
                dma((5,)),
                pltpu.SemaphoreType.REGULAR,
                pltpu.SemaphoreType.REGULAR,
            ],
            compiler_params=pltpu.CompilerParams(
                collective_id=0, has_side_effects=True, vmem_limit_bytes=48 * 2**20
            ),
            name="serve",
        )(master_down, *(pltpu.with_memory_space_constraint(a, pltpu.HBM) for a in (router_weight.T, router_gain[None, :])))
        final_down, scale_down, router = pl.pallas_call(
            place,
            out_shape=shapes,
            in_specs=[pl.BlockSpec(memory_space=pl.ANY)] * 3,
            out_specs=(hbm,) * 3,
            scratch_shapes=[dma((3,))],
            compiler_params=pltpu.CompilerParams(vmem_limit_bytes=8 * 2**20),
            name="place",
        )(*results)
        return final_down, scale_down, router.T

    return jax.shard_map(
        shards,
        mesh=mesh,
        in_specs=(
            P(("trial", "ep"), None, "fsdp"),
            P(("trial", "fsdp"), "ep"),
            P(("trial", "fsdp")),
        ),
        out_specs=(P(("trial", "ep"), "fsdp", None), P(("trial", "ep"), "fsdp"), P("trial", None)),
        check_vma=False,
    )
```

```python
import functools

import jax
import jax.numpy as jnp
from jax import lax
from jax.experimental import pallas as pl
from jax.experimental.pallas import tpu as pltpu
from jax.sharding import PartitionSpec as P

MESH = pl.DeviceIdType.MESH

OFFSETS = [(1, dx, dc) for dx in (2, 1, 3, 0) for dc in (0, 1)] + [
    (0, dx, dc) for dx in (1, 3, 2, 0) for dc in (0, 1) if (dx, dc) != (0, 0)
]
ALONG_X = [(0, dx, 0) for dx in (1, 3, 2)]
ACROSS_Z = (1, 0, 0)
PARTNER = (0, 0, 1)
ACROSS = OFFSETS[:8]
FIRST = 3
RAW = (2, 1)
WINDOW = 4
LEFT = 2


def kernel(
    experts,
    rows,
    w_hbm,
    rt_hbm,
    gain_hbm,
    final_ref,
    scale_ref,
    router_ref,
    w,
    narrow,
    raw,
    maxima,
    straight,
    early,
    partner,
    paired,
    along,
    planed,
    across,
    scales,
    rt,
    gain,
    own_router,
    load_sem,
    send_sem,
    recv_sem,
    raw_send,
    raw_recv,
    straight_send,
    straight_recv,
    pair_send,
    pair_recv,
    along_send,
    along_recv,
    across_send,
    across_recv,
    back_send,
    back_recv,
    router_send,
    router_recv,
    go,
    gate,
):
    trial, ep, me = lax.axis_index("trial"), lax.axis_index("ep"), lax.axis_index("fsdp")
    z_first = trial < 2
    plane, x, core = me // 8, lax.rem(me // 2, 4), lax.rem(me, 2)
    share = rows // 16
    last = experts - 1

    def at(offset, sign=1):
        dz, dx, dc = offset
        return lax.rem(plane + dz, 2) * 8 + lax.rem(x + 4 + sign * dx, 4) * 2 + lax.rem(core + dc, 2)

    def send(src, dst, send, recv, index, row=None):
        return pltpu.make_async_remote_copy(
            src_ref=src,
            dst_ref=dst,
            send_sem=send,
            recv_sem=recv,
            device_id=(trial, ep if row is None else row, index),
            device_id_type=MESH,
        )

    def columns(index):
        return pl.ds(pl.multiple_of(index * 128, 128), 128)

    def part_of(index):
        return pl.ds(pl.multiple_of(index * share, share), share)

    barrier = pltpu.get_barrier_semaphore()
    for o in OFFSETS:
        pl.semaphore_signal(barrier, inc=1, device_id=(trial, ep, at(o)), device_id_type=MESH)
    for d in (1, 2, 3):
        pl.semaphore_signal(barrier, inc=1, device_id=(trial, lax.rem(ep + d, 4), me), device_id_type=MESH)
    sharers = [(lax.rem(trial + 2, 4), ep, at(o)) for o in ((0, 0, 0), ACROSS_Z)]
    gated = lax.rem(me + 8 * lax.rem(trial, 2), 16)
    for d in sharers:
        pl.semaphore_signal(barrier, inc=1, device_id=d, device_id_type=MESH)

    loads = [pltpu.make_async_copy(w_hbm.at[e], w.at[e], load_sem.at[e]) for e in range(experts)]
    rt_load = pltpu.make_async_copy(rt_hbm, rt, load_sem.at[experts])
    gain_load = pltpu.make_async_copy(gain_hbm, gain, load_sem.at[experts + 1])
    for e in range(FIRST):
        loads[e].start()
    rt_load.start()
    gain_load.start()
    loads[last].start()
    for e in range(FIRST, last):
        loads[e].start()

    def take_maxima(e):
        for b in range(rows // 128):
            block = jnp.abs(w[e, b * 128 : (b + 1) * 128, :])
            maxima[e, b : b + 1, :] = jnp.max(block.T, axis=0, keepdims=True)

    def divide(e, scale):
        inverse = 1.0 / scale
        for b in range(rows // 128):
            factor = jnp.broadcast_to(inverse[b : b + 1, :], (128, 128)).T
            narrow[e, b * 128 : (b + 1) * 128, :] = (w[e, b * 128 : (b + 1) * 128, :] * factor).astype(jnp.bfloat16)

    def maxima_of(lo, hi):
        def one(e, carry):
            pltpu.make_async_copy(w_hbm.at[e], w.at[e], load_sem.at[e]).wait()
            take_maxima(e)
            return carry

        lax.fori_loop(lo, hi, one, 0)

    with jax.named_scope("first_maxima"):
        maxima_of(0, FIRST)
    with jax.named_scope("router_part"):
        rt_load.wait()
        gain_load.wait()
        part = (rt[...] * gain[...]).astype(jnp.bfloat16)
        own_router[...] = part
        own_rows = pl.ds(pl.multiple_of(ep * 16, 16), 16)
        router_ref[own_rows, columns(me)] = part
    loads[last].wait()

    def other_maxima():
        with jax.named_scope("other_maxima"):
            maxima_of(FIRST, last)
            take_maxima(last)

    straights = [
        send(maxima.at[e], straight.at[e, i], straight_send.at[e], straight_recv.at[e], at(o))
        for e in range(FIRST)
        for i, o in enumerate(OFFSETS)
    ]
    raws = [
        send(w.at[last, part_of(at(o)), :], raw.at[i], raw_send, raw_recv, at(o))
        for i, o in enumerate(ACROSS)
    ]
    router_y = [
        send(own_router, router_ref.at[own_rows, columns(me)], router_send.at[0], router_recv.at[0], me, lax.rem(ep + d, 4))
        for d in (1, 2, 3)
    ]
    router_z = send(own_router, router_ref.at[own_rows, columns(me)], router_send.at[1], router_recv.at[1], at(ACROSS_Z))
    half = experts // 2
    mine, theirs = pl.ds(core * half, half), pl.ds((1 - core) * half, half)
    pair = send(maxima.at[theirs], partner, pair_send, pair_recv, at(PARTNER))
    along_x = [send(planed, along.at[i], along_send, along_recv, at(o)) for i, o in enumerate(ALONG_X)]
    across_z = send(paired, across, across_send, across_recv, at(ACROSS_Z))
    back = send(scales.at[mine], scales.at[mine], back_send, back_recv, at(PARTNER))

    @pl.when(jnp.logical_not(z_first))
    def _():
        other_maxima()

    with jax.named_scope("barrier_wait"):
        pl.semaphore_wait(barrier, len(OFFSETS) + 3 + len(sharers))

    @pl.when(z_first)
    def _():
        for s in straights + raws[: RAW[0]] + router_y + [router_z]:
            s.start()
        other_maxima()
        pair.start()

    @pl.when(jnp.logical_not(z_first))
    def _():
        for s in [pair] + router_y + [router_z]:
            s.start()

    with jax.named_scope("pair"):
        pair.wait()
        paired[...] = jnp.maximum(maxima[mine], partner[...])
    across_z.start()

    @pl.when(jnp.logical_not(z_first))
    def _():
        with jax.named_scope("gate_open"):
            across_z.wait_send()
            router_z.wait_send()
            pl.semaphore_signal(gate, inc=1, device_id=(lax.rem(trial + 2, 4), ep, gated), device_id_type=MESH)
            for s in raws[: RAW[1]]:
                s.start()

    everyone = list(enumerate(OFFSETS))
    far, near = everyone[:8], everyone[8:]

    def parcel(e, i, o):
        block = pl.ds(e, 1)
        return send(
            narrow.at[block, part_of(at(o)), :],
            final_ref.at[block, :, columns(me)],
            send_sem.at[lax.rem(e, WINDOW), i // 8],
            recv_sem.at[i],
            at(o),
        )

    def await_sent(e, which):
        if which:
            size = narrow.at[0, pl.ds(0, share * len(which)), :]
            send(size, size, send_sem.at[lax.rem(e, WINDOW), which[0][0] // 8], recv_sem.at[0], me).wait_send()

    def step(e, which):
        with jax.named_scope("send_wait"):
            if not isinstance(e, int):
                @pl.when(e >= WINDOW)
                def _():
                    await_sent(e, which)

        for i, o in which:
            parcel(e, i, o).start()

    def fresh(e, scale):
        with jax.named_scope("divide"):
            divide(e, scale)
        final_ref[e, :, columns(me)] = narrow[e, part_of(me), :]

    def steps(lo, hi, which, first):
        def one(e, carry):
            if first:
                fresh(e, scales[e])
            step(e, which)
            return carry

        lax.fori_loop(lo, hi, one, 0)

    @pl.when(z_first)
    def _():
        for e in range(FIRST):
            with jax.named_scope("straight_wait"):
                send(straight.at[e], straight.at[e], straight_send.at[e], straight_recv.at[e], me).wait()
            top = maxima[e]
            for i in range(len(OFFSETS)):
                top = jnp.maximum(top, straight[e, i])
            early[e] = top
            fresh(e, early[e])
            if e == 0:
                with jax.named_scope("gate_wait"):
                    pl.semaphore_wait(gate, 1)
            step(e, far)
        across_z.wait_send()

    with jax.named_scope("across"):
        across_z.wait_recv()
        planed[...] = jnp.maximum(paired[...], across[...])
    for s in along_x:
        s.start()
    with jax.named_scope("along"):
        send(along, along, along_send, along_recv, me).wait()
        top = planed[...]
        for i in range(len(ALONG_X)):
            top = jnp.maximum(top, along[i])
        scales[mine] = top
    back.start()
    with jax.named_scope("back"):
        back.wait()

    ours = scales[:, pl.ds(me // 2, 1), :].reshape(experts, 128)
    scale_ref[...] = jnp.where(core == 0, ours[:, :share], ours[:, share:])

    opposite = lax.rem(me + 8, 16)
    theirs_y = router_ref.at[own_rows, columns(opposite)]
    router_y2 = [
        send(theirs_y, theirs_y, router_send.at[2], router_recv.at[2], me, lax.rem(ep + d, 4)) for d in (1, 2, 3)
    ]
    router_x = [
        send(router_ref.at[:, columns(c)], router_ref.at[:, columns(c)], router_send.at[3], router_recv.at[3], at(o))
        for c in (me, opposite)
        for o in ALONG_X
    ]
    router_core = [
        send(router_ref.at[:, columns(c)], router_ref.at[:, columns(c)], router_send.at[4], router_recv.at[4], at(PARTNER))
        for c in [i * 2 + core for i in range(8)]
    ]

    def finish_router():
        with jax.named_scope("router_rest"):
            def arrived(which, blocks, columns_of):
                size = router_ref.at[pl.ds(0, 16 * blocks), pl.ds(0, 128 * columns_of)]
                send(size, size, router_send.at[which], router_recv.at[which], me).wait()

            arrived(0, 3, 1)
            router_z.wait_recv()
            for s in router_y2:
                s.start()
            arrived(2, 3, 1)
            for s in router_x:
                s.start()
            arrived(3, 4, 6)
            for s in router_core:
                s.start()
            arrived(4, 4, 8)

    def take_raw(count):
        with jax.named_scope("raw"):
            factor = jnp.broadcast_to(1.0 / ours[last:], (128, 128)).T
            factor = jnp.where(core == 0, factor[:share], factor[share:])
            if count:
                size = raw.at[pl.ds(0, count)]
                send(size, size, raw_send, raw_recv, me).wait()
            for i, o in enumerate(ACROSS[:count]):
                final_ref[last, :, columns(at(o, -1))] = (raw[i] * factor).astype(jnp.bfloat16)

    def received(which, count):
        for i, o in which:
            whole = final_ref.at[pl.ds(0, count), :, columns(at(o, -1))]
            send(whole, whole, send_sem.at[0, 0], recv_sem.at[i], at(o)).wait_recv()

    @pl.when(z_first)
    def _():
        with jax.named_scope("far_first"):
            steps(FIRST, last, far, True)
            fresh(last, scales[last])
            await_sent(last - WINDOW, far)
            for i, o in far[RAW[0] :]:
                parcel(last, i, o).start()
        with jax.named_scope("far_sent"):
            router_z.wait_send()
            for e in range(last - WINDOW + 1, last - LEFT + 1):
                await_sent(e, far)
            for d in sharers:
                pl.semaphore_signal(go, inc=1, device_id=d, device_id_type=MESH)
        take_raw(RAW[0])
        finish_router()
        with jax.named_scope("near_second"):
            steps(0, experts, near, False)
        with jax.named_scope("last_sends"):
            for e in range(last - LEFT + 1, last):
                await_sent(e, far)
            await_sent(last, far[RAW[0] :])
            for e in range(experts - WINDOW, experts):
                await_sent(e, near)
        with jax.named_scope("last_far"):
            received(far[: RAW[0]], last)
            received(far[RAW[0] :], experts)

    @pl.when(jnp.logical_not(z_first))
    def _():
        with jax.named_scope("near_first"):
            steps(0, experts, near, True)
        finish_router()
        with jax.named_scope("go_wait"):
            pl.semaphore_wait(go, len(sharers))
        with jax.named_scope("far_second"):
            steps(0, last, far, False)
            await_sent(last - WINDOW, far)
            for i, o in far[RAW[1] :]:
                parcel(last, i, o).start()
        take_raw(RAW[1])
        with jax.named_scope("last_sends"):
            for e in range(experts - WINDOW, experts):
                await_sent(e, near)
            for e in range(last - WINDOW + 1, last):
                await_sent(e, far)
            await_sent(last, far[RAW[1] :])
        with jax.named_scope("last_far"):
            received(far[: RAW[1]], last)
            received(far[RAW[1] :], experts)

    with jax.named_scope("last_near"):
        received(near, experts)


def place(final_in, scale_in, router_in, final_out, scale_out, router_out, sem):
    copies = [
        pltpu.make_async_copy(src, dst, sem.at[i])
        for i, (src, dst) in enumerate(((final_in, final_out), (scale_in, scale_out), (router_in, router_out)))
    ]
    for c in copies:
        c.start()
    for c in copies:
        c.wait()


def solution(mesh):
    def shards(master_down, router_weight, router_gain):
        experts, rows, _ = master_down.shape
        held = experts // 2
        peers, sides = len(OFFSETS), len(ALONG_X)
        vmem = pl.BlockSpec(memory_space=pltpu.VMEM)
        hbm = pl.BlockSpec(memory_space=pltpu.HBM)
        dma = pltpu.SemaphoreType.DMA
        shapes = (
            jax.ShapeDtypeStruct((experts, rows // 16, 2048), jnp.bfloat16),
            jax.ShapeDtypeStruct((experts, rows // 16), jnp.float32),
            jax.ShapeDtypeStruct((64, 2048), jnp.bfloat16),
        )
        tile = (8, 128)
        results = pl.pallas_call(
            functools.partial(kernel, experts, rows),
            out_shape=shapes,
            in_specs=[hbm] * 3,
            out_specs=(vmem, vmem, vmem),
            scratch_shapes=[
                pltpu.VMEM((experts, rows, 128), jnp.float32),
                pltpu.VMEM((experts, rows, 128), jnp.bfloat16),
                pltpu.VMEM((len(ACROSS), rows // 16, 128), jnp.float32),
                pltpu.VMEM((experts, *tile), jnp.float32),
                pltpu.VMEM((FIRST, peers, *tile), jnp.float32),
                pltpu.VMEM((FIRST, *tile), jnp.float32),
                pltpu.VMEM((held, *tile), jnp.float32),
                pltpu.VMEM((held, *tile), jnp.float32),
                pltpu.VMEM((sides, held, *tile), jnp.float32),
                pltpu.VMEM((held, *tile), jnp.float32),
                pltpu.VMEM((held, *tile), jnp.float32),
                pltpu.VMEM((experts, *tile), jnp.float32),
                pltpu.VMEM((16, 128), jnp.float32),
                pltpu.VMEM((1, 128), jnp.float32),
                pltpu.VMEM((16, 128), jnp.bfloat16),
                dma((experts + 2,)),
                dma((WINDOW, 2)),
                dma((peers,)),
                dma,
                dma,
                dma((FIRST,)),
                dma((FIRST,)),
                *[dma] * 8,
                dma((5,)),
                dma((5,)),
                pltpu.SemaphoreType.REGULAR,
                pltpu.SemaphoreType.REGULAR,
            ],
            compiler_params=pltpu.CompilerParams(
                collective_id=0, has_side_effects=True, vmem_limit_bytes=48 * 2**20
            ),
            name="serve",
        )(master_down, *(pltpu.with_memory_space_constraint(a, pltpu.HBM) for a in (router_weight.T, router_gain[None, :])))
        final_down, scale_down, router = pl.pallas_call(
            place,
            out_shape=shapes,
            in_specs=[pl.BlockSpec(memory_space=pl.ANY)] * 3,
            out_specs=(hbm,) * 3,
            scratch_shapes=[dma((3,))],
            compiler_params=pltpu.CompilerParams(vmem_limit_bytes=8 * 2**20),
            name="place",
        )(*results)
        return final_down, scale_down, router.T

    return jax.shard_map(
        shards,
        mesh=mesh,
        in_specs=(
            P(("trial", "ep"), None, "fsdp"),
            P(("trial", "fsdp"), "ep"),
            P(("trial", "fsdp")),
        ),
        out_specs=(P(("trial", "ep"), "fsdp", None), P(("trial", "ep"), "fsdp"), P("trial", None)),
        check_vma=False,
    )
```
